128 devices in a mesh: member: 4 (over y, x), mp: 32 (over z, core).
Axes of the slice: x: 2, y: 2, z: 16, core: 2. Of those that a mesh axis runs over, the one named last changes fastest.
The devices are a block of a 8x8x16 slice.
Arguments:
- nodes: bfloat16 [8192, 4096], P(('member', 'mp')), parts along dimension 0, may hold values from -6 to 6
- norm_gain: float32 [4096], replicated, may hold values from 0.1 to 1.9
- w_in: bfloat16 [4096, 16384], P(None, 'mp'), may hold values from -0.09375 to 0.09375
- b_in: float32 [16384], P('mp'), may hold values from -3 to 3
- w_out: bfloat16 [16384, 4096], P('mp'), may hold values from -0.046875 to 0.046875
- b_out: float32 [4096], replicated, may hold values from -3 to 3
Outputs:
- updated: bfloat16 [8192, 4096], P(('member', 'mp')), parts along dimension 0
The draws below stay inside these ranges and needn't reach their ends.
There are 4 independent parts, one for each index of `member`. The reference program is written for one: setup_inputs(seed, part) draws one part's arguments, and reference() takes and returns one part's arrays. A program takes and returns all parts, laid end to end along the dimension named above; an argument that names none is the same for every part. Nothing has to cross between parts.
All inputs are finite; a program needn't handle non-finite values.
Results may differ from the reference program's by a relative error of at most 0.015.
Values may be sent and summed in bfloat16 or wider, within the bound.
A program may use at most 128 MiB of HBM per device.

```python
import jax
import jax.numpy as jnp
from jax import lax

D = 4096
FF = 16384
ROWS = 2048
N_MP = 32


def levels(key, extent, pieces, low, high):
    loudness = 1.0
    for dim, blocks in pieces:
        draws = jax.random.uniform(jax.random.fold_in(jax.random.fold_in(key, 6), dim), (blocks,), jnp.float32, low / len(pieces), high / len(pieces))
        loudness = loudness * jnp.repeat(jnp.exp(draws), extent[dim] // blocks).reshape((-1,) + (1,) * (len(extent) - 1 - dim))
    return loudness


def gaussian(key, shape, deviation, limit, cuts=(), kind=jnp.bfloat16):
    drawn = deviation * jax.random.normal(key, shape, jnp.float32)
    if cuts:
        drawn = drawn * levels(key, shape, cuts, -0.22, 0.18)
    return jnp.clip(drawn, -limit, limit).astype(kind)


def setup_inputs(seed: int = 0, part: int = 0) -> dict:
    key_list = jax.random.split(jax.random.key(seed), 7)
    own_keys = jax.random.split(jax.random.fold_in(key_list[6], part), 7)
    return {
        "nodes": gaussian(own_keys[0], (ROWS, D), 1.0, 6.0, ((0, 32),)),
        "norm_gain": jnp.clip(1.0 + 0.18 * jax.random.normal(key_list[1], (D,), jnp.float32), 0.1, 1.9),
        "w_in": gaussian(key_list[2], (D, FF), D ** -0.5, 0.09375, ((1, 32),)),
        "b_in": gaussian(key_list[3], (FF,), 0.5, 3.0, ((0, 32),), jnp.float32),
        "w_out": gaussian(key_list[4], (FF, D), FF ** -0.5, 0.046875, ((0, 32),)),
        "b_out": gaussian(key_list[5], (D,), 0.5, 3.0, (), jnp.float32),
    }


def reference(nodes, norm_gain, w_in, b_in, w_out, b_out):
    values = nodes.astype(jnp.float32)
    mean = lax.optimization_barrier(jnp.mean(values, axis=1, keepdims=True))
    var = lax.optimization_barrier(jnp.mean((values - mean) ** 2, axis=1, keepdims=True))
    normed = ((values - mean) / jnp.sqrt(var + 1e-05) * norm_gain).astype(jnp.bfloat16)
    pre = jnp.dot(normed, w_in, preferred_element_type=jnp.float32) + b_in
    hidden = jax.nn.gelu(pre, approximate=True).astype(jnp.bfloat16)
    width = FF // N_MP

    def add_share(index, total):
        start = (index * width).astype(jnp.int32)
        left = lax.dynamic_slice_in_dim(hidden, start, width, 1)
        right = lax.dynamic_slice_in_dim(w_out, start, width, 0)
        share = jnp.dot(left, right, preferred_element_type=jnp.float32).astype(jnp.bfloat16)
        return total + share.astype(jnp.float32)
    mlp_out = lax.fori_loop(jnp.int32(0), jnp.int32(N_MP), add_share, jnp.zeros((nodes.shape[0], nodes.shape[1]), jnp.float32))
    return (values + mlp_out + b_out).astype(jnp.bfloat16)
```

```python
import functools
import math

import jax
import jax.numpy as jnp
from jax import lax
from jax.experimental import pallas as pl
from jax.experimental.pallas import tpu as pltpu
from jax.sharding import PartitionSpec as P

MESH = pl.DeviceIdType.MESH
WAVES = 2
PARTS = 2
PIECES = 4
RIGHT, LEFT = 0, 1
GATHER, SCATTER = 0, 1


def gelu(v):
    return 0.5 * v * (1.0 + jnp.tanh(math.sqrt(2.0 / math.pi) * (v + 0.044715 * (v * v * v))))


def kernel(
    devices, nodes_hbm, gain_hbm, w_in_hbm, b_in_hbm, w_out_hbm, b_out_hbm, out,
    nodes, gain, b_in, b_out, w_in, w_out, rows, hidden, partial, sums,
    load_sem, swap_send, swap_recv, send_sem, recv_sem,
):
    ring = devices // 2
    half = ring // 2
    _, _, _, height, width = rows.shape
    depth = width * PARTS
    units = w_in.shape[2]

    me = lax.axis_index("mp")
    core = lax.rem(me, 2)
    sibling = me + 1 - 2 * core
    to = (lax.rem(me + 2, devices), lax.rem(me + devices - 2, devices))

    def cols(q):
        return pl.ds(q * width, width)

    def hops(q, d):
        return half if (q < PARTS // 2) == (d == RIGHT) else half - 1

    def from_behind(k, d):
        return k if d == RIGHT else lax.rem(ring - k, ring)

    def ahead(j, d):
        return lax.rem(ring - j, ring) if d == RIGHT else j

    def gather_copy(w, k, q, d):
        return pltpu.make_async_remote_copy(
            src_ref=rows.at[w, from_behind(k - 1, d), q],
            dst_ref=rows.at[w, from_behind(k, d), q],
            send_sem=send_sem.at[GATHER, w, d, q, lax.rem(k, 2)],
            recv_sem=recv_sem.at[GATHER, w, d, q, k - 1],
            device_id={"mp": to[d]},
            device_id_type=MESH,
        )

    def scatter_copy(w, k, q, d, first=False):
        j = hops(q, d) + 1 - k
        source = partial.at[w, ahead(j, d), q] if first else sums.at[w, d, j, q]
        return pltpu.make_async_remote_copy(
            src_ref=source,
            dst_ref=sums.at[w, d, j - 1, q],
            send_sem=send_sem.at[SCATTER, w, d, q, lax.rem(k, 2)],
            recv_sem=recv_sem.at[SCATTER, w, d, q, k - 1],
            device_id={"mp": to[d]},
            device_id_type=MESH,
        )

    def begin(phase, w):
        for q in range(PARTS):
            for d in (RIGHT, LEFT):
                if phase == GATHER:
                    gather_copy(w, 1, q, d).start()
                else:
                    scatter_copy(w, 1, q, d, first=True).start()

    def finish_rows(w, q):
        lines = slice(w * height, (w + 1) * height)
        total = (
            nodes[lines, cols(q)].astype(jnp.float32)
            + partial[w, 0, q].astype(jnp.float32)
            + sums[w, RIGHT, 0, q].astype(jnp.float32)
            + sums[w, LEFT, 0, q].astype(jnp.float32)
            + b_out[:, cols(q)]
        )
        out[lines, cols(q)] = total.astype(out.dtype)

    def events(phase, w, k, work=None):
        static = isinstance(k, int)
        for q in range(PARTS):
            for d in (RIGHT, LEFT):
                last = hops(q, d)
                if static and k > last:
                    continue
                copy = gather_copy if phase == GATHER else scatter_copy
                if phase == SCATTER and static and k == 1:
                    copy = functools.partial(scatter_copy, first=True)
                copy(w, k, q, d).wait_recv()
                if static and k == last:
                    if phase == SCATTER and last == half:
                        finish_rows(w, q)
                else:
                    if phase == SCATTER:
                        j = last - k
                        sums[w, d, j, q] = (
                            sums[w, d, j, q].astype(jnp.float32)
                            + partial[w, ahead(j, d), q].astype(jnp.float32)
                        ).astype(sums.dtype)
                    if not static or k > 1:
                        wait_sent(phase, w, k - 1, q, d)
                    copy = gather_copy if phase == GATHER else scatter_copy
                    copy(w, k + 1, q, d).start()
            if work is not None:
                for n in range(q * PIECES // PARTS, (q + 1) * PIECES // PARTS):
                    work(n)

    def wait_sent(phase, w, k, q, d):
        if phase == GATHER:
            gather_copy(w, k, q, d).wait_send()
        else:
            scatter_copy(w, k, q, d, first=True).wait_send()

    def drain(phase, w):
        for q in range(PARTS):
            for d in (RIGHT, LEFT):
                for k in (hops(q, d) - 1, hops(q, d)):
                    wait_sent(phase, w, k, q, d)

    def loop(low, high, body):
        def step(k, carry):
            body(k)
            return carry

        lax.fori_loop(low, high, step, 0)

    slots = ring // 2
    band = slots * height
    tile = 2 * units // PIECES
    step = depth // (2 * PIECES)

    def first_layer(w, m, n):
        h, c = divmod(n * tile, units)
        pre = b_in[h, :, c : c + tile]
        for q in range(PARTS):
            x = rows[w, pl.ds(m * slots, slots), q].reshape(band, width)
            pre = pre + jnp.dot(
                x, w_in[h, q * width : (q + 1) * width, c : c + tile], preferred_element_type=jnp.float32
            )
        hidden[pl.ds(m * band, band), n * tile : (n + 1) * tile] = gelu(pre).astype(hidden.dtype)

    def second_layer(w, m, n):
        x = hidden[pl.ds(m * band, band), :]
        for c in (2 * n * step, (2 * n + 1) * step):
            share = jnp.dot(
                x,
                w_out[:, :, c : c + step].reshape(2 * units, step),
                preferred_element_type=jnp.float32,
            )
            q, c = divmod(c, width)
            partial[w, pl.ds(m * slots, slots), q, :, c : c + step] = share.reshape(
                slots, height, step
            ).astype(partial.dtype)

    def normalize(w):
        for r in range(height // 16):
            lines = slice(w * height + r * 16, w * height + (r + 1) * 16)
            values = nodes[lines, :].astype(jnp.float32)
            mean = jnp.mean(values, axis=1, keepdims=True)
            centred = values - mean
            var = jnp.mean(centred * centred, axis=1, keepdims=True)
            scaled = (centred * lax.rsqrt(var + 1e-05) * gain[...]).astype(rows.dtype)
            for q in range(PARTS):
                rows[w, 0, q, r * 16 : (r + 1) * 16, :] = scaled[:, q * width : (q + 1) * width]

    loads = [
        pltpu.make_async_copy(source, target, load_sem.at[i])
        for i, (source, target) in enumerate(
            (
                (nodes_hbm.at[:height], nodes.at[:height]),
                (gain_hbm, gain),
                (nodes_hbm.at[height:], nodes.at[height:]),
                (b_in_hbm, b_in.at[0]),
                (b_out_hbm, b_out),
                (w_in_hbm, w_in.at[0]),
                (w_out_hbm, w_out.at[0]),
            )
        )
    ]
    swaps = [
        pltpu.make_async_remote_copy(
            src_ref=source,
            dst_ref=target,
            send_sem=swap_send.at[i],
            recv_sem=swap_recv.at[i],
            device_id={"mp": sibling},
            device_id_type=MESH,
        )
        for i, (source, target) in enumerate(
            ((w_in_hbm, w_in.at[1]), (w_out_hbm, w_out.at[1]), (b_in_hbm, b_in.at[1]))
        )
    ]

    barrier = pltpu.get_barrier_semaphore()
    for other in (*to, sibling):
        pl.semaphore_signal(barrier, inc=1, device_id={"mp": other}, device_id_type=MESH)
    for load in loads:
        load.start()
    loads[0].wait()
    loads[1].wait()
    normalize(0)
    pl.semaphore_wait(barrier, 3)

    begin(GATHER, 0)
    loads[2].wait()
    normalize(1)
    begin(GATHER, 1)
    for swap in swaps:
        swap.start()
    events(GATHER, 0, 1)
    loop(2, half - 1, lambda k: events(GATHER, 0, k))
    events(GATHER, 1, 1)
    events(GATHER, 0, half - 1)
    events(GATHER, 1, 2)
    events(GATHER, 0, half)
    drain(GATHER, 0)
    for load in loads[3:]:
        load.wait()
    for swap in swaps:
        swap.wait()

    def compute_beside(phase, w, compute, k0):
        loop(k0, k0 + 2, lambda k: events(phase, w, k, lambda q: first_layer(compute, k - k0, q)))
        loop(k0 + 2, k0 + 4, lambda k: events(phase, w, k, lambda q: second_layer(compute, k - k0 - 2, q)))
        if k0 + 4 < half - 1:
            loop(k0 + 4, half - 1, lambda k: events(phase, w, k))

    compute_beside(GATHER, 1, 0, 3)
    begin(SCATTER, 0)
    events(GATHER, 1, half - 1)
    events(SCATTER, 0, 1)
    events(GATHER, 1, half)
    drain(GATHER, 1)
    compute_beside(SCATTER, 0, 1, 2)
    begin(SCATTER, 1)
    events(SCATTER, 0, half - 1)
    events(SCATTER, 1, 1)
    events(SCATTER, 0, half)
    drain(SCATTER, 0)
    loop(2, half - 1, lambda k: events(SCATTER, 1, k))
    events(SCATTER, 1, half - 1)
    events(SCATTER, 1, half)
    drain(SCATTER, 1)


def solution(mesh):
    devices = mesh.shape["mp"]

    def local(nodes, norm_gain, w_in, b_in, w_out, b_out):
        total, depth = nodes.shape
        units = w_in.shape[1]
        ring, height = devices // 2, total // WAVES
        half = ring // 2
        bf16, f32 = jnp.bfloat16, jnp.float32
        in_hbm = pl.BlockSpec(memory_space=pltpu.HBM)
        return pl.pallas_call(
            functools.partial(kernel, devices),
            out_shape=jax.ShapeDtypeStruct((total, depth), bf16),
            in_specs=[in_hbm] * 6,
            out_specs=pl.BlockSpec(memory_space=pltpu.VMEM),
            scratch_shapes=[
                pltpu.VMEM((total, depth), bf16),
                pltpu.VMEM((1, depth), f32),
                pltpu.VMEM((2, 1, units), f32),
                pltpu.VMEM((1, depth), f32),
                pltpu.VMEM((2, depth, units), bf16),
                pltpu.VMEM((2, units, depth), bf16),
                pltpu.VMEM((WAVES, ring, PARTS, height, depth // PARTS), bf16),
                pltpu.VMEM((ring * height, 2 * units), bf16),
                pltpu.VMEM((WAVES, ring, PARTS, height, depth // PARTS), bf16),
                pltpu.VMEM((WAVES, 2, half, PARTS, height, depth // PARTS), bf16),
                pltpu.SemaphoreType.DMA((7,)),
                pltpu.SemaphoreType.DMA((3,)),
                pltpu.SemaphoreType.DMA((3,)),
                pltpu.SemaphoreType.DMA((2, WAVES, 2, PARTS, 2)),
                pltpu.SemaphoreType.DMA((2, WAVES, 2, PARTS, half)),
            ],
            compiler_params=pltpu.CompilerParams(
                collective_id=0, has_side_effects=True, vmem_limit_bytes=48 * 2**20
            ),
        )(
            *(
                pltpu.with_memory_space_constraint(x, pltpu.HBM)
                for x in (
                    nodes,
                    norm_gain.reshape(1, depth),
                    w_in,
                    b_in.reshape(1, units),
                    w_out,
                    b_out.reshape(1, depth),
                )
            )
        )

    return jax.shard_map(
        local,
        mesh=mesh,
        in_specs=(P(("member", "mp"), None), P(), P(None, "mp"), P("mp"), P("mp", None), P()),
        out_specs=P(("member", "mp"), None),
        check_vma=False,
    )
```

```python
import functools
import math

import jax
import jax.numpy as jnp
from jax import lax
from jax.experimental import pallas as pl
from jax.experimental.pallas import tpu as pltpu
from jax.sharding import PartitionSpec as P

MESH = pl.DeviceIdType.MESH
WAVES = 2
PARTS = 2
PIECES = 4
RIGHT, LEFT = 0, 1
GATHER, SCATTER = 0, 1
ORDER = [pair for i in range(PARTS) for pair in ((i, RIGHT), (PARTS - 1 - i, LEFT))]


def gelu(v):
    return 0.5 * v * (1.0 + jnp.tanh(math.sqrt(2.0 / math.pi) * (v + 0.044715 * (v * v * v))))


def kernel(
    devices, nodes_hbm, gain_hbm, w_in_hbm, b_in_hbm, w_out_hbm, b_out_hbm, out,
    nodes, gain, b_in, b_out, w_in, w_out, rows, hidden, partial, sums,
    load_sem, swap_send, swap_recv, send_sem, recv_sem,
):
    ring = devices // 2
    half = ring // 2
    _, _, _, height, width = rows.shape
    depth = width * PARTS
    units = w_in.shape[2]

    me = lax.axis_index("mp")
    core = lax.rem(me, 2)
    sibling = me + 1 - 2 * core
    to = (lax.rem(me + 2, devices), lax.rem(me + devices - 2, devices))

    def cols(q):
        return pl.ds(q * width, width)

    def hops(q, d):
        return half if (q < PARTS // 2) == (d == RIGHT) else half - 1

    def from_behind(k, d):
        return k if d == RIGHT else lax.rem(ring - k, ring)

    def ahead(j, d):
        return lax.rem(ring - j, ring) if d == RIGHT else j

    def gather_copy(w, k, q, d):
        return pltpu.make_async_remote_copy(
            src_ref=rows.at[w, from_behind(k - 1, d), q],
            dst_ref=rows.at[w, from_behind(k, d), q],
            send_sem=send_sem.at[GATHER, w, d, q, lax.rem(k, 2)],
            recv_sem=recv_sem.at[GATHER, w, d, q, k - 1],
            device_id={"mp": to[d]},
            device_id_type=MESH,
        )

    def scatter_copy(w, k, q, d, first=False):
        j = hops(q, d) + 1 - k
        source = partial.at[w, ahead(j, d), q] if first else sums.at[w, d, j, q]
        return pltpu.make_async_remote_copy(
            src_ref=source,
            dst_ref=sums.at[w, d, j - 1, q],
            send_sem=send_sem.at[SCATTER, w, d, q, lax.rem(k, 2)],
            recv_sem=recv_sem.at[SCATTER, w, d, q, k - 1],
            device_id={"mp": to[d]},
            device_id_type=MESH,
        )

    def begin(phase, w):
        for q, d in ORDER:
            if phase == GATHER:
                gather_copy(w, 1, q, d).start()
            else:
                scatter_copy(w, 1, q, d, first=True).start()

    def finish_rows(w, q):
        lines = slice(w * height, (w + 1) * height)
        total = (
            nodes[lines, cols(q)].astype(jnp.float32)
            + partial[w, 0, q].astype(jnp.float32)
            + sums[w, RIGHT, 0, q].astype(jnp.float32)
            + sums[w, LEFT, 0, q].astype(jnp.float32)
            + b_out[:, cols(q)]
        )
        out[lines, cols(q)] = total.astype(out.dtype)

    def events(phase, w, k, work=None):
        static = isinstance(k, int)
        for i, (q, d) in enumerate(ORDER):
            last = hops(q, d)
            if static and k > last:
                continue
            copy = gather_copy if phase == GATHER else scatter_copy
            if phase == SCATTER and static and k == 1:
                copy = functools.partial(scatter_copy, first=True)
            copy(w, k, q, d).wait_recv()
            if static and k == last:
                if phase == SCATTER and last == half:
                    finish_rows(w, q)
            else:
                if phase == SCATTER:
                    j = last - k
                    sums[w, d, j, q] = (
                        sums[w, d, j, q].astype(jnp.float32)
                        + partial[w, ahead(j, d), q].astype(jnp.float32)
                    ).astype(sums.dtype)
                if not static or k > 1:
                    wait_sent(phase, w, k - 1, q, d)
                copy = gather_copy if phase == GATHER else scatter_copy
                copy(w, k + 1, q, d).start()
            if work is not None and i % (len(ORDER) // PIECES) == 0:
                work(i * PIECES // len(ORDER))

    def wait_sent(phase, w, k, q, d):
        if phase == GATHER:
            gather_copy(w, k, q, d).wait_send()
        else:
            scatter_copy(w, k, q, d, first=True).wait_send()

    def drain(phase, w):
        for q in range(PARTS):
            for d in (RIGHT, LEFT):
                for k in (hops(q, d) - 1, hops(q, d)):
                    wait_sent(phase, w, k, q, d)

    def loop(low, high, body):
        def step(k, carry):
            body(k)
            return carry

        lax.fori_loop(low, high, step, 0)

    slots = ring // 2
    band = slots * height
    tile = 2 * units // PIECES
    step = depth // (2 * PIECES)

    def first_layer(w, m, n):
        h, c = divmod(n * tile, units)
        pre = b_in[h, :, c : c + tile]
        for q in range(PARTS):
            x = rows[w, pl.ds(m * slots, slots), q].reshape(band, width)
            pre = pre + jnp.dot(
                x, w_in[h, q * width : (q + 1) * width, c : c + tile], preferred_element_type=jnp.float32
            )
        hidden[pl.ds(m * band, band), n * tile : (n + 1) * tile] = gelu(pre).astype(hidden.dtype)

    def second_layer(w, m, n):
        x = hidden[pl.ds(m * band, band), :]
        for c in (2 * n * step, (2 * n + 1) * step):
            share = jnp.dot(
                x,
                w_out[:, :, c : c + step].reshape(2 * units, step),
                preferred_element_type=jnp.float32,
            )
            q, c = divmod(c, width)
            partial[w, pl.ds(m * slots, slots), q, :, c : c + step] = share.reshape(
                slots, height, step
            ).astype(partial.dtype)

    def normalize(w):
        for r in range(height // 16):
            lines = slice(w * height + r * 16, w * height + (r + 1) * 16)
            values = nodes[lines, :].astype(jnp.float32)
            mean = jnp.mean(values, axis=1, keepdims=True)
            centred = values - mean
            var = jnp.mean(centred * centred, axis=1, keepdims=True)
            scaled = (centred * lax.rsqrt(var + 1e-05) * gain[...]).astype(rows.dtype)
            for q in range(PARTS):
                rows[w, 0, q, r * 16 : (r + 1) * 16, :] = scaled[:, q * width : (q + 1) * width]

    loads = [
        pltpu.make_async_copy(source, target, load_sem.at[i])
        for i, (source, target) in enumerate(
            (
                (nodes_hbm.at[:height], nodes.at[:height]),
                (gain_hbm, gain),
                (nodes_hbm.at[height:], nodes.at[height:]),
                (b_in_hbm, b_in.at[0]),
                (b_out_hbm, b_out),
                (w_in_hbm, w_in.at[0]),
                (w_out_hbm, w_out.at[0]),
            )
        )
    ]
    swaps = [
        pltpu.make_async_remote_copy(
            src_ref=source,
            dst_ref=target,
            send_sem=swap_send.at[i],
            recv_sem=swap_recv.at[i],
            device_id={"mp": sibling},
            device_id_type=MESH,
        )
        for i, (source, target) in enumerate(
            ((w_in_hbm, w_in.at[1]), (w_out_hbm, w_out.at[1]), (b_in_hbm, b_in.at[1]))
        )
    ]

    barrier = pltpu.get_barrier_semaphore()
    for other in (*to, sibling):
        pl.semaphore_signal(barrier, inc=1, device_id={"mp": other}, device_id_type=MESH)
    for load in loads:
        load.start()
    loads[0].wait()
    loads[1].wait()
    normalize(0)
    pl.semaphore_wait(barrier, 3)

    begin(GATHER, 0)
    loads[2].wait()
    normalize(1)
    begin(GATHER, 1)
    for swap in swaps:
        swap.start()
    events(GATHER, 0, 1)
    loop(2, half - 1, lambda k: events(GATHER, 0, k))
    events(GATHER, 1, 1)
    events(GATHER, 0, half - 1)
    events(GATHER, 1, 2)
    events(GATHER, 0, half)
    drain(GATHER, 0)
    for load in loads[3:]:
        load.wait()
    for swap in swaps:
        swap.wait()

    def compute_beside(phase, w, compute, k0):
        loop(k0, k0 + 2, lambda k: events(phase, w, k, lambda q: first_layer(compute, k - k0, q)))
        loop(k0 + 2, k0 + 4, lambda k: events(phase, w, k, lambda q: second_layer(compute, k - k0 - 2, q)))
        if k0 + 4 < half - 1:
            loop(k0 + 4, half - 1, lambda k: events(phase, w, k))

    compute_beside(GATHER, 1, 0, 3)
    begin(SCATTER, 0)
    events(GATHER, 1, half - 1)
    events(SCATTER, 0, 1)
    events(GATHER, 1, half)
    drain(GATHER, 1)
    compute_beside(SCATTER, 0, 1, 2)
    begin(SCATTER, 1)
    events(SCATTER, 0, half - 1)
    events(SCATTER, 1, 1)
    events(SCATTER, 0, half)
    drain(SCATTER, 0)
    loop(2, half - 1, lambda k: events(SCATTER, 1, k))
    events(SCATTER, 1, half - 1)
    events(SCATTER, 1, half)
    drain(SCATTER, 1)


def solution(mesh):
    devices = mesh.shape["mp"]

    def local(nodes, norm_gain, w_in, b_in, w_out, b_out):
        total, depth = nodes.shape
        units = w_in.shape[1]
        ring, height = devices // 2, total // WAVES
        half = ring // 2
        bf16, f32 = jnp.bfloat16, jnp.float32
        in_hbm = pl.BlockSpec(memory_space=pltpu.HBM)
        return pl.pallas_call(
            functools.partial(kernel, devices),
            out_shape=jax.ShapeDtypeStruct((total, depth), bf16),
            in_specs=[in_hbm] * 6,
            out_specs=pl.BlockSpec(memory_space=pltpu.VMEM),
            scratch_shapes=[
                pltpu.VMEM((total, depth), bf16),
                pltpu.VMEM((1, depth), f32),
                pltpu.VMEM((2, 1, units), f32),
                pltpu.VMEM((1, depth), f32),
                pltpu.VMEM((2, depth, units), bf16),
                pltpu.VMEM((2, units, depth), bf16),
                pltpu.VMEM((WAVES, ring, PARTS, height, depth // PARTS), bf16),
                pltpu.VMEM((ring * height, 2 * units), bf16),
                pltpu.VMEM((WAVES, ring, PARTS, height, depth // PARTS), bf16),
                pltpu.VMEM((WAVES, 2, half, PARTS, height, depth // PARTS), bf16),
                pltpu.SemaphoreType.DMA((7,)),
                pltpu.SemaphoreType.DMA((3,)),
                pltpu.SemaphoreType.DMA((3,)),
                pltpu.SemaphoreType.DMA((2, WAVES, 2, PARTS, 2)),
                pltpu.SemaphoreType.DMA((2, WAVES, 2, PARTS, half)),
            ],
            compiler_params=pltpu.CompilerParams(
                collective_id=0, has_side_effects=True, vmem_limit_bytes=48 * 2**20
            ),
        )(
            *(
                pltpu.with_memory_space_constraint(x, pltpu.HBM)
                for x in (
                    nodes,
                    norm_gain.reshape(1, depth),
                    w_in,
                    b_in.reshape(1, units),
                    w_out,
                    b_out.reshape(1, depth),
                )
            )
        )

    return jax.shard_map(
        local,
        mesh=mesh,
        in_specs=(P(("member", "mp"), None), P(), P(None, "mp"), P("mp"), P("mp", None), P()),
        out_specs=P(("member", "mp"), None),
        check_vma=False,
    )
```
